32 devices in a mesh: facet: 4 (over z), half: 4 (over x, core), sub: 2 (over y).
Axes of the slice: x: 2, y: 2, z: 4, core: 2. Of those that a mesh axis runs over, the one named last changes fastest.
Arguments:
- facets: bfloat16 [4, 2, 2048, 2048], P('facet', None, ('half', 'sub')), may hold values from -6 to 6
- weights: float32 [512, 16, 512], P('facet', ('half', 'sub')), may hold values from 0.25 to 4
- facet_offsets: int32 [4, 2], replicated, may hold values from 0 to 511
- subgrid_offsets: int32 [16], replicated, may hold values from 0 to 2047
- column: int32 [1], replicated, may hold values from 0 to 2047
Outputs:
- facet_update: bfloat16 [4, 2, 2048, 2048], P('facet', None, ('half', 'sub'))
- spectra: float32 [512, 16, 2, 512], P('facet', ('half', 'sub'))
The draws below stay inside these ranges and needn't reach their ends.
All inputs are finite; a program needn't handle non-finite values.
Results may differ from the reference program's by a relative error of at most 0.025.
Values may be sent and summed in bfloat16 or wider, within the bound.
No kernel may reach another device: no remote copies, remote signals or barrier semaphores. Data moves between devices by JAX's collectives and lax.ppermute only.
A program may use at most 128 MiB of HBM per device.

```python
import math
import jax
import jax.numpy as jnp
from jax import lax

YF = 2048
M = 128
XM = 512
SUBS = 16
FACETS = 4


def plant(drawn, stream_key, least, high):
    extent = drawn.shape
    spot = [jax.random.randint(jax.random.fold_in(stream_key, axis), (), 0, extent[axis]) for axis in range(len(extent))]
    drawn = drawn.at[tuple(spot)].set(least)
    longest = extent.index(max(extent))
    spot[longest] = (spot[longest] + 1) % extent[longest]
    return drawn.at[tuple(spot)].set(high)


def block_levels(key, dims, cuts, smallest, high):
    loudness, own = 1.0, jax.random.fold_in(key, 6)
    for position, parts in cuts:
        heights = jnp.exp(jax.random.uniform(jax.random.fold_in(own, position), (parts,), jnp.float32, smallest / len(cuts), high / len(cuts)))
        loudness = loudness * jnp.repeat(heights, dims[position] // parts).reshape([-1 if axis == position else 1 for axis in range(len(dims))])
    return loudness


def bell_draw(key, extent, scale, most, shards=(), held_as=jnp.bfloat16):
    result = scale * jax.random.normal(key, extent, jnp.float32)
    if shards:
        result = result * block_levels(key, extent, shards, -0.22, 0.18)
    return jnp.clip(result, -most, most).astype(held_as)


def setup_inputs(seed: int = 0) -> dict:
    key_list = jax.random.split(jax.random.key(seed), 6)
    return {
        "facets": bell_draw(key_list[0], (FACETS, 2, YF, YF), 1.0, 6.0, ((0, 4), (2, 8))),
        "weights": jnp.clip(jnp.exp(math.log(4.0) - 2.7725887 * jax.random.uniform(key_list[1], (XM, SUBS, XM), jnp.float32) ** block_levels(key_list[1], (XM, SUBS, XM), ((0, 4), (1, 8)), -0.2, 0.2)), 0.25, 4.0),
        "facet_offsets": plant(jax.random.randint(key_list[2], (FACETS, 2), 0, XM), jax.random.fold_in(key_list[2], 1), 0, XM - 1).astype(jnp.int32),
        "subgrid_offsets": plant(jax.random.randint(key_list[3], (SUBS,), 0, YF), jax.random.fold_in(key_list[3], 1), 0, YF - 1).astype(jnp.int32),
        "column": jax.random.randint(key_list[4], (1,), 0, YF).astype(jnp.int32),
    }


HI = lax.Precision.HIGHEST

def wave(freq, pos, n):
    turns = freq[:, None] * pos[None, :] % n
    angle = turns.astype(jnp.float32) * (2.0 * math.pi / n)
    return (jnp.cos(angle), jnp.sin(angle))

def facet_table(freq, pos, n):
    cosine, sine = wave(freq, pos, n)
    shaped = (jnp.sin(math.pi * (pos.astype(jnp.float32) + 0.5) / n) ** 2)[None, :] / math.sqrt(n)
    return ((cosine * shaped).astype(jnp.bfloat16), (-sine * shaped).astype(jnp.bfloat16))

def cmat(form, l_real, l_imag, r_real, r_imag):
    real = jnp.einsum(form, l_real, r_real, precision=HI) - jnp.einsum(form, l_imag, r_imag, precision=HI)
    imag = jnp.einsum(form, l_real, r_imag, precision=HI) + jnp.einsum(form, l_imag, r_real, precision=HI)
    return (real, imag)

def reference(facets, weights, facet_offsets, subgrid_offsets, column):
    near = jnp.arange(M, dtype=jnp.int32)
    span = jnp.arange(XM, dtype=jnp.int32)
    every = jnp.arange(YF, dtype=jnp.int32)
    column_freq = (column[0] + near) % YF
    q_real, q_imag = facet_table(column_freq, every, YF)
    sub_freq = ((subgrid_offsets[:, None] + near[None, :]) % YF).reshape(-1)
    p_real, p_imag = facet_table(sub_freq, every, YF)
    scale = 1.0 / math.sqrt(XM)
    cos_f, sin_f = wave(span, span, XM)
    f_real = cos_f * scale
    f_imag = -sin_f * scale

    def place(offset):
        rows = (span[:, None] == ((offset[0] + near) % XM)[None, :]).astype(jnp.float32)
        cols = (span[:, None] == ((offset[1] + near) % XM)[None, :]).astype(jnp.float32)
        return (rows, cols)

    def forward(carry, item):
        planes, offset = item
        f32 = jnp.float32
        a_real = (jnp.dot(planes[0], q_real.T, preferred_element_type=f32) - jnp.dot(planes[1], q_imag.T, preferred_element_type=f32)).astype(jnp.bfloat16)
        a_imag = (jnp.dot(planes[0], q_imag.T, preferred_element_type=f32) + jnp.dot(planes[1], q_real.T, preferred_element_type=f32)).astype(jnp.bfloat16)
        c_real = (jnp.dot(p_real, a_real, preferred_element_type=f32) - jnp.dot(p_imag, a_imag, preferred_element_type=f32)).reshape(SUBS, M, M)
        c_imag = (jnp.dot(p_real, a_imag, preferred_element_type=f32) + jnp.dot(p_imag, a_real, preferred_element_type=f32)).reshape(SUBS, M, M)
        rows, cols = place(offset)
        g_real = carry[0] + jnp.einsum('aj,sjk,bk->sab', rows, c_real, cols, precision=HI)
        g_imag = carry[1] + jnp.einsum('aj,sjk,bk->sab', rows, c_imag, cols, precision=HI)
        return ((g_real, g_imag), None)
    start = (jnp.zeros((SUBS, XM, XM), jnp.float32), jnp.zeros((SUBS, XM, XM), jnp.float32))
    (g_real, g_imag), _ = lax.scan(forward, start, (facets, facet_offsets))
    t_real, t_imag = cmat('ab,sbc->sac', f_real, f_imag, g_real, g_imag)
    hat_real, hat_imag = cmat('sac,cd->sad', t_real, t_imag, f_real, f_imag)
    resident = jnp.transpose(weights, (1, 0, 2))
    h_real = resident * hat_real
    h_imag = resident * hat_imag
    spectra = jnp.transpose(jnp.stack([h_real, h_imag], 1), (2, 0, 1, 3))
    u_real, u_imag = cmat('ab,sbc->sac', f_real, -f_imag, h_real, h_imag)
    space_real, space_imag = cmat('sac,cd->sad', u_real, u_imag, f_real, -f_imag)
    gain = 2.0 * math.sqrt(YF / M)

    def backward(offset):
        f32 = jnp.float32
        rows, cols = place(offset)
        d_real = jnp.einsum('aj,sab,bk->sjk', rows, space_real, cols, precision=HI).astype(jnp.bfloat16).reshape(SUBS * M, M)
        d_imag = jnp.einsum('aj,sab,bk->sjk', rows, space_imag, cols, precision=HI).astype(jnp.bfloat16).reshape(SUBS * M, M)
        e_real = (jnp.dot(p_real.T, d_real, preferred_element_type=f32) + jnp.dot(p_imag.T, d_imag, preferred_element_type=f32)).astype(jnp.bfloat16)
        e_imag = (jnp.dot(p_real.T, d_imag, preferred_element_type=f32) - jnp.dot(p_imag.T, d_real, preferred_element_type=f32)).astype(jnp.bfloat16)
        w_real = jnp.dot(e_real, q_real, preferred_element_type=f32) + jnp.dot(e_imag, q_imag, preferred_element_type=f32)
        w_imag = jnp.dot(e_imag, q_real, preferred_element_type=f32) - jnp.dot(e_real, q_imag, preferred_element_type=f32)
        return (jnp.stack([w_real, w_imag]) * gain).astype(jnp.bfloat16)
    update = lax.map(backward, facet_offsets)
    return (update, spectra)
```

```python
import math

import jax
import jax.numpy as jnp
from jax import lax
from jax.experimental import pallas as pl
from jax.experimental.pallas import tpu as pltpu
from jax.sharding import PartitionSpec as P

YF = 2048
M = 128
XM = 512
STEP = 16
F32 = jnp.float32
BF = jnp.bfloat16
TEAM = ("half", "sub")

SIN = [(-1) ** i * math.pi ** (2 * i + 1) / math.factorial(2 * i + 1) for i in range(6)]
COS = [(-1) ** i * math.pi ** (2 * i) / math.factorial(2 * i) for i in range(7)]


def poly(coefs, u):
    out = coefs[-1] * u + coefs[-2]
    for c in coefs[-3::-1]:
        out = out * u + c
    return out


def circle(turns):
    x = turns - jnp.floor(turns + 0.5)
    u = x * x
    s = poly(SIN, u) * x
    c = poly(COS, u)
    return 1.0 - 2.0 * (s * s), 2.0 * (s * c)


def iota(shape, axis):
    return lax.broadcasted_iota(jnp.int32, shape, axis).astype(F32)


def turn_by(a, b):
    return a[0] * b[0] - a[1] * b[1], a[1] * b[0] + a[0] * b[1]


def taper(pos):
    return 0.5 - 0.5 * circle((pos + 0.5) * (1.0 / YF))[0]


def fine_rows(pos, n, amp):
    c, s = circle(iota((STEP, pos.shape[1]), 0) * pos * (1.0 / n))
    return c * amp, s * amp


def freq_rows(offset, pos, n, fine, store):
    count = M // STEP
    coarse = circle((offset + STEP * iota((count, pos.shape[1]), 0)) * pos * (1.0 / n))
    for a in range(count):
        store(a * STEP, *turn_by((coarse[0][a : a + 1], coarse[1][a : a + 1]), fine))


def freq_lanes(offset, base, rows, n, amp, store):
    freq = offset + iota((1, M), 1)
    fine = circle(iota((STEP, M), 0) * freq * (1.0 / n))
    count = rows // STEP
    coarse = circle((base + STEP * iota((count, M), 0)) * freq * (1.0 / n))
    for a in range(count):
        c, s = turn_by((coarse[0][a : a + 1], coarse[1][a : a + 1]), fine)
        w = amp(a * STEP)
        store(a * STEP, c * w, s * w)


def dot(a, b):
    return lax.dot_general(a, b, (((1,), (0,)), ((), ())), preferred_element_type=F32)


def dot_nt(a, b):
    return lax.dot_general(a, b, (((1,), (1,)), ((), ())), preferred_element_type=F32)


def vmem():
    return pl.BlockSpec(memory_space=pltpu.VMEM)


def smem():
    return pl.BlockSpec(memory_space=pltpu.SMEM)


def call(kernel, name, ins, outs, in_specs, scratch=(), flops=0, limit=None):
    return pl.pallas_call(
        kernel,
        name=name,
        out_shape=[jax.ShapeDtypeStruct(s, d) for s, d in outs],
        in_specs=in_specs,
        out_specs=[vmem() for _ in outs],
        scratch_shapes=list(scratch),
        cost_estimate=pl.CostEstimate(flops=flops, bytes_accessed=1 << 20, transcendentals=0),
        compiler_params=pltpu.CompilerParams(vmem_limit_bytes=limit),
    )(*ins)


def team_layout():
    half, sub = lax.axis_size("half"), lax.axis_size("sub")
    low = 2 if half % 2 == 0 else 1
    return half // low, low, sub


def member(dh, dl, ds):
    high, low, sub = team_layout()
    h, s = lax.axis_index("half"), lax.axis_index("sub")
    hi = lax.rem(h // low + high - dh, high)
    lo = lax.rem(lax.rem(h, low) + low - dl, low)
    return (hi * low + lo) * sub + lax.rem(s + sub - ds, sub)


def steps():
    high, low, sub = team_layout()
    return [(dh, ds) for dh in range(high) for ds in range(sub)]


def send(value, dh, dl, ds):
    high, low, sub = team_layout()
    pairs = []
    for hi in range(high):
        for lo in range(low):
            for s in range(sub):
                to = ((hi + dh) % high * low + (lo + dl) % low) * sub + (s + ds) % sub
                pairs.append(((hi * low + lo) * sub + s, to))
    return lax.ppermute(value, TEAM, pairs)


def a_kernel(column, x, q, a, xbuf, sem):
    rows = x.shape[1]
    copies = [pltpu.make_async_copy(x.at[i], xbuf.at[i], sem.at[i]) for i in range(2)]
    for c in copies:
        c.start()
    off = column[0].astype(F32)
    width = 512
    for i in range(YF // width):
        pos = iota((1, width), 1) + float(i * width)
        fine = fine_rows(pos, YF, taper(pos) * (1.0 / math.sqrt(YF)))
        cols = slice(i * width, (i + 1) * width)

        def store(r, c, s):
            q[r : r + STEP, cols] = c.astype(BF)
            q[M + r : M + r + STEP, cols] = (-s).astype(BF)

        freq_rows(off, pos, YF, fine, store)
    copies[0].wait()
    fr = dot_nt(xbuf[0], q[...])
    copies[1].wait()
    fi = dot_nt(xbuf[1], q[...])
    a[:, :M] = (fr[:, :M] - fi[:, M:]).astype(BF)
    a[:, M:] = (fr[:, M:] + fi[:, :M]).astype(BF)


def p_kernel(sub_here, rows_here, subs, p_re, p_im):
    low = team_layout()[1]
    for q, (dh, ds) in enumerate(steps()):
        base = (member(dh, 0, ds) * rows_here).astype(F32)
        pos = iota((1, rows_here), 1) + base
        fine = fine_rows(pos, YF, taper(pos) * (1.0 / math.sqrt(YF)))
        cols = slice(q * rows_here, (q + 1) * rows_here)
        for p in range(low):
            for s in range(sub_here):
                off = subs[member(0, p, 0) * sub_here + s].astype(F32)

                def store(r, c, sn):
                    at = (p * sub_here + s) * M + r
                    p_re[at : at + STEP, cols] = c.astype(BF)
                    p_im[at : at + STEP, cols] = (-sn).astype(BF)

                freq_rows(off, pos, YF, fine, store)


def pt_kernel(sub_here, rows_here, subs, p_re, p_im, w):
    low = team_layout()[1]
    for p in range(low):
        base = (member(0, p, 0) * rows_here).astype(F32)
        w[...] = taper(iota((rows_here, M), 0) + base) * (1.0 / math.sqrt(YF))
        for q, (dh, ds) in enumerate(steps()):
            for s in range(sub_here):
                off = subs[member(dh, 0, ds) * sub_here + s].astype(F32)
                cols = slice((q * sub_here + s) * M, (q * sub_here + s + 1) * M)

                def store(r, c, sn):
                    at = p * rows_here + r
                    p_re[at : at + STEP, cols] = c.astype(BF)
                    p_im[at : at + STEP, cols] = (-sn).astype(BF)

                freq_lanes(off, base, rows_here, YF, lambda r: w[r : r + STEP, :], store)


def row_kernel(offs, r, w):
    off = offs[2 * lax.axis_index("facet")].astype(F32)
    scale = 1.0 / math.sqrt(XM)

    def store_r(at, c, s):
        r[0, at : at + STEP, :M] = c.astype(BF)
        r[0, at : at + STEP, M:] = s.astype(BF)
        r[1, at : at + STEP, :M] = (-s).astype(BF)
        r[1, at : at + STEP, M:] = c.astype(BF)

    freq_lanes(off, 0.0, XM, XM, lambda _: scale, store_r)

    def store_w(at, c, s):
        w[at : at + STEP, :] = c.astype(BF)
        w[M + at : M + at + STEP, :] = s.astype(BF)

    pos = iota((1, XM), 1)
    freq_rows(off, pos, XM, fine_rows(pos, XM, scale), store_w)


def col_kernel(count, offs, col):
    pos = iota((1, XM), 1)
    fine = fine_rows(pos, XM, 1.0 / math.sqrt(XM))

    def facet(f, _):
        def store(at, c, s):
            top = pl.ds(pl.multiple_of(f * 2 * M + at, STEP), STEP)
            low = pl.ds(pl.multiple_of(f * 2 * M + M + at, STEP), STEP)
            c, s = c.astype(BF), s.astype(BF)
            col[top, :XM] = c
            col[top, XM:] = -s
            col[low, :XM] = s
            col[low, XM:] = c

        freq_rows(offs[2 * f + 1].astype(F32), pos, XM, fine, store)
        return 0

    lax.fori_loop(0, count, facet, 0)


def c_kernel(sub_here, part, *refs):
    blocks, (p_re, p_im, out) = refs[:-3], refs[-3:]
    rows_here = blocks[0].shape[0]
    at = slice(part * sub_here * M, (part + 1) * sub_here * M)
    re = im = 0.0
    for q, a in enumerate(blocks):
        cols = slice(q * rows_here, (q + 1) * rows_here)
        re = re + dot(p_re[at, cols], a[...])
        im = im + dot(p_im[at, cols], a[...])
    c_re = re[:, :M] - im[:, M:]
    c_im = re[:, M:] + im[:, :M]
    for s in range(sub_here):
        rows = slice(s * M, (s + 1) * M)
        out[:M, rows] = c_re[rows].astype(out.dtype)
        out[M:, rows] = c_im[rows].astype(out.dtype)


def k_kernel(*refs):
    parts, (r, out) = refs[:-2], refs[-2:]
    total = parts[0][...]
    for p in parts[1:]:
        total = total + p[...].astype(F32)
    total = total.astype(BF)
    nf, sub_here, rows, _ = out.shape
    for c in range(2):
        k = dot(r[c], total).astype(BF)
        for s in range(sub_here):
            out[:, s, :, c * M : (c + 1) * M] = k[:, s * M : (s + 1) * M].reshape(nf, rows, M)


def spectrum_kernel(got, weights, col, spectra, out):
    nf, sub_here, rows, _ = got.shape
    acc = 0.0
    for f in range(nf):
        acc = acc + dot(got[f].reshape(sub_here * rows, 2 * M), col[f * 2 * M : (f + 1) * 2 * M, :])
    w = weights[...].reshape(sub_here * rows, XM)
    re = acc[:, :XM] * w
    im = acc[:, XM:] * w
    for s in range(sub_here):
        spectra[s, 0] = re[s * rows : (s + 1) * rows]
        spectra[s, 1] = im[s * rows : (s + 1) * rows]
    re, im = re.astype(BF), im.astype(BF)
    for f in range(nf):
        at = slice(f * 2 * M, (f + 1) * 2 * M)
        y = dot_nt(re, col[at, :XM]) + dot_nt(im, col[at, XM:])
        out[f] = y.astype(BF).reshape(sub_here, rows, 2 * M)


def d_kernel(back, w, out):
    nf, sub_here, rows, _ = back.shape
    for s in range(sub_here):
        t = dot(w[...], back[:, s].reshape(nf * rows, 2 * M))
        at = slice(s * M, (s + 1) * M)
        out[at, :M] = (t[:M, :M] - t[M:, M:]).astype(BF)
        out[at, M:] = (t[:M, M:] + t[M:, :M]).astype(BF)


def e_kernel(part, *refs):
    blocks, (p_re, p_im, out) = refs[:-3], refs[-3:]
    rows_here, depth = out.shape[0], blocks[0].shape[0]
    at = slice(part * rows_here, (part + 1) * rows_here)
    re = im = 0.0
    for q, d in enumerate(blocks):
        cols = slice(q * depth, (q + 1) * depth)
        re = re + dot(p_re[at, cols], d[...])
        im = im + dot(p_im[at, cols], d[...])
    out[:, :M] = (re[:, :M] + im[:, M:]).astype(out.dtype)
    out[:, M:] = (re[:, M:] - im[:, :M]).astype(out.dtype)


def update_kernel(*refs):
    parts, (q, out) = refs[:-2], refs[-2:]
    e = parts[0][...]
    for p in parts[1:]:
        e = e + p[...].astype(F32)
    e = e.astype(BF)
    turned = jnp.concatenate([e[:, M:], -e[:, :M]], 1)
    gain = 2.0 * math.sqrt(YF / M)
    width = 512
    for i in range(YF // width):
        cols = slice(i * width, (i + 1) * width)
        out[0, 0, :, cols] = (dot(e, q[:, cols]) * gain).astype(BF)
        out[0, 1, :, cols] = (dot(turned, q[:, cols]) * gain).astype(BF)


def bind(kernel, *args):
    def body(*refs):
        kernel(*args, *refs)

    return body


def shards(facets, weights, facet_offsets, subgrid_offsets, column):
    planes = facets[0]
    rows_here = planes.shape[1]
    block_rows, sub_here, _ = weights.shape
    nf = facet_offsets.shape[0]
    high, low, sub = team_layout()
    group = high * sub
    offs = facet_offsets.reshape(-1)
    limit = 20 << 20 if nf <= 4 else 56 << 20
    side = sub_here * M
    wide = (rows_here, 2 * M)

    q, a = call(
        a_kernel,
        "facet_columns",
        (column, planes),
        [((2 * M, YF), BF), (wide, BF)],
        [smem(), pl.BlockSpec(memory_space=pl.ANY)],
        [pltpu.VMEM(planes.shape, BF), pltpu.SemaphoreType.DMA((2,))],
        flops=8 * rows_here * YF * M,
        limit=limit,
    )
    blocks = [a] + [send(a, dh, 0, ds) for dh, ds in steps()[1:]]
    shape = (low * side, group * rows_here)
    p_re, p_im = call(
        bind(p_kernel, sub_here, rows_here),
        "p_table",
        (subgrid_offsets,),
        [(shape, BF), (shape, BF)],
        [smem()],
        flops=1 << 29,
        limit=limit,
    )
    r, w = call(
        row_kernel,
        "row_table",
        (offs,),
        [((2, XM, 2 * M), BF), ((2 * M, XM), BF)],
        [smem()],
        flops=1 << 28,
        limit=limit,
    )
    (col,) = call(
        bind(col_kernel, nf),
        "col_table",
        (offs,),
        [((nf * 2 * M, 2 * XM), BF)],
        [smem()],
        flops=1 << 29,
        limit=limit,
    )
    shape = (low * rows_here, group * side)
    pt_re, pt_im = call(
        bind(pt_kernel, sub_here, rows_here),
        "pt_table",
        (subgrid_offsets,),
        [(shape, BF), (shape, BF)],
        [smem()],
        [pltpu.VMEM((rows_here, M), F32)],
        flops=1 << 29,
        limit=limit,
    )
    parts = []
    for p in [*range(1, low), 0]:
        (c,) = call(
            bind(c_kernel, sub_here, p),
            f"contrib_{p}",
            (*blocks, p_re, p_im),
            [((2 * M, side), BF if p else F32)],
            [vmem()] * (group + 2),
            flops=8 * side * group * rows_here * M,
            limit=limit,
        )
        parts.append(send(c, 0, (low - p) % low, 0) if p else c)
    parts = parts[-1:] + parts[:-1]
    cube = (nf, sub_here, block_rows, 2 * M)
    (k,) = call(
        k_kernel,
        "row_spectra",
        (*parts, r),
        [(cube, BF)],
        [vmem()] * (low + 1),
        flops=8 * XM * M * side,
        limit=limit,
    )
    got = lax.all_to_all(k, "facet", split_axis=0, concat_axis=0, tiled=True)
    spectra, y = call(
        spectrum_kernel,
        "weighted_spectra",
        (got, jnp.transpose(weights, (1, 0, 2)), col),
        [((sub_here, 2, block_rows, XM), F32), (cube, BF)],
        [vmem()] * 3,
        flops=16 * sub_here * block_rows * nf * M * XM,
        limit=limit,
    )
    back = lax.all_to_all(y, "facet", split_axis=0, concat_axis=0, tiled=True)
    (d,) = call(
        d_kernel,
        "windows",
        (back, w),
        [((side, 2 * M), BF)],
        [vmem()] * 2,
        flops=8 * XM * M * side,
        limit=limit,
    )
    blocks = [d] + [send(d, dh, 0, ds) for dh, ds in steps()[1:]]
    parts = []
    for p in [*range(1, low), 0]:
        (e,) = call(
            bind(e_kernel, p),
            f"rows_{p}",
            (*blocks, pt_re, pt_im),
            [(wide, BF if p else F32)],
            [vmem()] * (group + 2),
            flops=8 * rows_here * group * side * M,
            limit=limit,
        )
        parts.append(send(e, 0, (low - p) % low, 0) if p else e)
    parts = parts[-1:] + parts[:-1]
    (update,) = call(
        update_kernel,
        "facet_update",
        (*parts, q),
        [((1, 2, rows_here, YF), BF)],
        [vmem()] * (low + 1),
        flops=8 * rows_here * YF * M,
        limit=limit,
    )
    return (update, jnp.transpose(spectra, (2, 0, 1, 3)))


def solution(mesh):
    return jax.shard_map(
        shards,
        mesh=mesh,
        in_specs=(
            P("facet", None, ("half", "sub"), None),
            P("facet", ("half", "sub"), None),
            P(),
            P(),
            P(),
        ),
        out_specs=(
            P("facet", None, ("half", "sub"), None),
            P("facet", ("half", "sub"), None, None),
        ),
        check_vma=False,
    )
```

```python
import math

import jax
import jax.numpy as jnp
from jax import lax
from jax.experimental import pallas as pl
from jax.experimental.pallas import tpu as pltpu
from jax.sharding import PartitionSpec as P

YF = 2048
M = 128
XM = 512
STEP = 16
F32 = jnp.float32
BF = jnp.bfloat16
TEAM = ("half", "sub")

SIN = [(-1) ** i * math.pi ** (2 * i + 1) / math.factorial(2 * i + 1) for i in range(6)]
COS = [(-1) ** i * math.pi ** (2 * i) / math.factorial(2 * i) for i in range(7)]


def poly(coefs, u):
    out = coefs[-1] * u + coefs[-2]
    for c in coefs[-3::-1]:
        out = out * u + c
    return out


def circle(turns):
    x = turns - jnp.floor(turns + 0.5)
    u = x * x
    s = poly(SIN, u) * x
    c = poly(COS, u)
    return 1.0 - 2.0 * (s * s), 2.0 * (s * c)


def iota(shape, axis):
    return lax.broadcasted_iota(jnp.int32, shape, axis).astype(F32)


def turn_by(a, b):
    return a[0] * b[0] - a[1] * b[1], a[1] * b[0] + a[0] * b[1]


def taper(pos):
    return 0.5 - 0.5 * circle((pos + 0.5) * (1.0 / YF))[0]


def fine_rows(pos, n, amp):
    c, s = circle(iota((STEP, pos.shape[1]), 0) * pos * (1.0 / n))
    return c * amp, s * amp


def freq_rows(offset, pos, n, fine, store):
    count = M // STEP
    coarse = circle((offset + STEP * iota((count, pos.shape[1]), 0)) * pos * (1.0 / n))
    for a in range(count):
        store(a * STEP, *turn_by((coarse[0][a : a + 1], coarse[1][a : a + 1]), fine))


def freq_lanes(offset, base, rows, n, amp, store):
    freq = offset + iota((1, M), 1)
    fine = circle(iota((STEP, M), 0) * freq * (1.0 / n))
    count = rows // STEP
    coarse = circle((base + STEP * iota((count, M), 0)) * freq * (1.0 / n))
    for a in range(count):
        c, s = turn_by((coarse[0][a : a + 1], coarse[1][a : a + 1]), fine)
        w = amp(a * STEP)
        store(a * STEP, c * w, s * w)


def dot(a, b):
    return lax.dot_general(a, b, (((1,), (0,)), ((), ())), preferred_element_type=F32)


def dot_nt(a, b):
    return lax.dot_general(a, b, (((1,), (1,)), ((), ())), preferred_element_type=F32)


def vmem():
    return pl.BlockSpec(memory_space=pltpu.VMEM)


def smem():
    return pl.BlockSpec(memory_space=pltpu.SMEM)


def hbm():
    return pl.BlockSpec(memory_space=pltpu.HBM)


def call(kernel, name, ins, outs, in_specs, scratch=(), flops=0, limit=None, out_spec=vmem):
    return pl.pallas_call(
        kernel,
        name=name,
        out_shape=[jax.ShapeDtypeStruct(s, d) for s, d in outs],
        in_specs=in_specs,
        out_specs=[out_spec() for _ in outs],
        scratch_shapes=list(scratch),
        cost_estimate=pl.CostEstimate(flops=flops, bytes_accessed=1 << 20, transcendentals=0),
        compiler_params=pltpu.CompilerParams(vmem_limit_bytes=limit),
    )(*ins)


def team_layout():
    half, sub = lax.axis_size("half"), lax.axis_size("sub")
    low = 2 if half % 2 == 0 else 1
    return half // low, low, sub


def member(dh, dl, ds):
    high, low, sub = team_layout()
    h, s = lax.axis_index("half"), lax.axis_index("sub")
    hi = lax.rem(h // low + high - dh, high)
    lo = lax.rem(lax.rem(h, low) + low - dl, low)
    return (hi * low + lo) * sub + lax.rem(s + sub - ds, sub)


def steps():
    high, low, sub = team_layout()
    return [(dh, ds) for dh in range(high) for ds in range(sub)]


def send(value, dh, dl, ds):
    high, low, sub = team_layout()
    pairs = []
    for hi in range(high):
        for lo in range(low):
            for s in range(sub):
                to = ((hi + dh) % high * low + (lo + dl) % low) * sub + (s + ds) % sub
                pairs.append(((hi * low + lo) * sub + s, to))
    return lax.ppermute(value, TEAM, pairs)


def a_kernel(column, x, q, a, xbuf, sem):
    rows = x.shape[1]
    copies = [pltpu.make_async_copy(x.at[i], xbuf.at[i], sem.at[i]) for i in range(2)]
    for c in copies:
        c.start()
    off = column[0].astype(F32)
    width = 512
    for i in range(YF // width):
        pos = iota((1, width), 1) + float(i * width)
        fine = fine_rows(pos, YF, taper(pos) * (1.0 / math.sqrt(YF)))
        cols = slice(i * width, (i + 1) * width)

        def store(r, c, s):
            q[r : r + STEP, cols] = c.astype(BF)
            q[M + r : M + r + STEP, cols] = (-s).astype(BF)

        freq_rows(off, pos, YF, fine, store)
    copies[0].wait()
    fr = dot_nt(xbuf[0], q[...])
    copies[1].wait()
    fi = dot_nt(xbuf[1], q[...])
    a[:, :M] = (fr[:, :M] - fi[:, M:]).astype(BF)
    a[:, M:] = (fr[:, M:] + fi[:, :M]).astype(BF)


def p_kernel(sub_here, rows_here, subs, p_re, p_im):
    low = team_layout()[1]
    for q, (dh, ds) in enumerate(steps()):
        base = (member(dh, 0, ds) * rows_here).astype(F32)
        pos = iota((1, rows_here), 1) + base
        fine = fine_rows(pos, YF, taper(pos) * (1.0 / math.sqrt(YF)))
        cols = slice(q * rows_here, (q + 1) * rows_here)
        for p in range(low):
            for s in range(sub_here):
                off = subs[member(0, p, 0) * sub_here + s].astype(F32)

                def store(r, c, sn):
                    at = (p * sub_here + s) * M + r
                    p_re[at : at + STEP, cols] = c.astype(BF)
                    p_im[at : at + STEP, cols] = (-sn).astype(BF)

                freq_rows(off, pos, YF, fine, store)


def pt_kernel(sub_here, rows_here, subs, p_re, p_im, w):
    low = team_layout()[1]
    for p in range(low):
        base = (member(0, p, 0) * rows_here).astype(F32)
        w[...] = taper(iota((rows_here, M), 0) + base) * (1.0 / math.sqrt(YF))
        for q, (dh, ds) in enumerate(steps()):
            for s in range(sub_here):
                off = subs[member(dh, 0, ds) * sub_here + s].astype(F32)
                cols = slice((q * sub_here + s) * M, (q * sub_here + s + 1) * M)

                def store(r, c, sn):
                    at = p * rows_here + r
                    p_re[at : at + STEP, cols] = c.astype(BF)
                    p_im[at : at + STEP, cols] = (-sn).astype(BF)

                freq_lanes(off, base, rows_here, YF, lambda r: w[r : r + STEP, :], store)


def peer(nf, i):
    return lax.bitwise_xor(lax.axis_index("facet"), i) if by_permutes(nf) else jnp.int32(i)


def by_permutes(nf):
    return nf in (2, 4)


def row_kernel(rows, offs, r, w):
    nf = offs.shape[1]
    off = offs[0, lax.axis_index("facet")].astype(F32)
    scale = 1.0 / math.sqrt(XM)
    for i in range(nf):
        base = (peer(nf, i) * rows).astype(F32)
        top = i * rows

        def store_r(at, c, s):
            at = at + top
            r[0, at : at + STEP, :M] = c.astype(BF)
            r[0, at : at + STEP, M:] = s.astype(BF)
            r[1, at : at + STEP, :M] = (-s).astype(BF)
            r[1, at : at + STEP, M:] = c.astype(BF)

        freq_lanes(off, base, rows, XM, lambda _: scale, store_r)

    if by_permutes(nf):
        base = [(peer(nf, i) * rows).astype(F32) for i in range(nf)]
        pos = jnp.concatenate([iota((1, rows), 1) + b for b in base], 1)
    else:
        pos = iota((1, XM), 1)

    def store_w(at, c, s):
        w[at : at + STEP, :] = c.astype(BF)
        w[M + at : M + at + STEP, :] = s.astype(BF)

    freq_rows(off, pos, XM, fine_rows(pos, XM, scale), store_w)


def col_kernel(offs, col):
    nf = offs.shape[1]
    pos = iota((1, XM), 1)
    fine = fine_rows(pos, XM, 1.0 / math.sqrt(XM))

    def facet(f, _):
        def store(at, c, s):
            top = pl.ds(pl.multiple_of(f * 2 * M + at, STEP), STEP)
            low = pl.ds(pl.multiple_of(f * 2 * M + M + at, STEP), STEP)
            c, s = c.astype(BF), s.astype(BF)
            col[top, :XM] = c
            col[top, XM:] = -s
            col[low, :XM] = s
            col[low, XM:] = c

        freq_rows(offs[1, peer(nf, f)].astype(F32), pos, XM, fine, store)
        return 0

    lax.fori_loop(0, nf, facet, 0)


def c_kernel(sub_here, part, *refs):
    blocks, (p_re, p_im, out) = refs[:-3], refs[-3:]
    rows_here = blocks[0].shape[0]
    at = slice(part * sub_here * M, (part + 1) * sub_here * M)
    re = im = 0.0
    for q, a in enumerate(blocks):
        cols = slice(q * rows_here, (q + 1) * rows_here)
        re = re + dot(p_re[at, cols], a[...])
        im = im + dot(p_im[at, cols], a[...])
    c_re = re[:, :M] - im[:, M:]
    c_im = re[:, M:] + im[:, :M]
    for s in range(sub_here):
        rows = slice(s * M, (s + 1) * M)
        out[:M, rows] = c_re[rows].astype(out.dtype)
        out[M:, rows] = c_im[rows].astype(out.dtype)


def k_kernel(low, s, *refs):
    parts, r, outs = refs[:low], refs[low], refs[low + 1 :]
    at = slice(s * M, (s + 1) * M)
    total = parts[0][:, at]
    for p in parts[1:]:
        total = total + p[:, at].astype(F32)
    total = total.astype(BF)
    for c in range(2):
        k = dot(r[c], total).astype(BF)
        put_blocks(outs, k, slice(c * M, (c + 1) * M))


def put_blocks(outs, value, lanes):
    if len(outs) == 1:
        outs[0][:, :, lanes] = value.reshape(outs[0].shape[0], -1, value.shape[1])
        return
    rows = outs[0].shape[0]
    for i, out in enumerate(outs):
        out[:, lanes] = value[i * rows : (i + 1) * rows]


def get_blocks(refs):
    if len(refs) == 1:
        return [refs[0][i] for i in range(refs[0].shape[0])]
    return [r[...] for r in refs]


def spectrum_kernel(count, s, sub_here, *refs):
    got, weights, col, spectrum, outs = refs[:count], refs[count], refs[count + 1], refs[count + 2], refs[count + 3 :]
    acc = 0.0
    for i, block in enumerate(get_blocks(got)):
        acc = acc + dot(block, col[i * 2 * M : (i + 1) * 2 * M, :])
    rows = acc.shape[0]
    groups = XM // 128
    w = jnp.concatenate(
        [weights[pl.ds(g * sub_here + s, rows, groups * sub_here), :] for g in range(groups)], 1
    )
    re = acc[:, :XM] * w
    im = acc[:, XM:] * w
    spectrum[0] = re
    spectrum[1] = im
    both = jnp.concatenate([re, im], 1).astype(BF)
    y = [dot_nt(both, col[i * 2 * M : (i + 1) * 2 * M, :]).astype(BF) for i in range(col.shape[0] // (2 * M))]
    put_blocks(outs, jnp.concatenate(y, 0), slice(0, 2 * M))


def spread_kernel(*refs):
    parts, (out, buf, sem) = refs[:-3], refs[-3:]
    rows = parts[0].shape[1]
    groups = XM // 128
    stride = len(parts) * groups * 2
    for s, part in enumerate(parts):
        for g in range(groups):
            for c in range(2):
                at = pl.ds((s * groups + g) * 2 + c, rows, stride)
                buf[at, :] = part[c, :, g * 128 : (g + 1) * 128]
    copy = pltpu.make_async_copy(buf, out, sem)
    copy.start()
    copy.wait()


def d_kernel(*refs):
    back, (w, out) = refs[:-2], refs[-2:]
    t = dot(w[...], jnp.concatenate(get_blocks(back), 0))
    out[:, :M] = (t[:M, :M] - t[M:, M:]).astype(BF)
    out[:, M:] = (t[:M, M:] + t[M:, :M]).astype(BF)


def e_kernel(part, sub_here, *refs):
    blocks, (p_re, p_im, out) = refs[:-3], refs[-3:]
    rows_here, depth = out.shape[0], sub_here * M
    at = slice(part * rows_here, (part + 1) * rows_here)
    re = im = 0.0
    for q in range(len(blocks) // sub_here):
        d = jnp.concatenate([b[...] for b in blocks[q * sub_here : (q + 1) * sub_here]], 0)
        cols = slice(q * depth, (q + 1) * depth)
        re = re + dot(p_re[at, cols], d)
        im = im + dot(p_im[at, cols], d)
    out[:, :M] = (re[:, :M] + im[:, M:]).astype(out.dtype)
    out[:, M:] = (re[:, M:] - im[:, :M]).astype(out.dtype)


def update_kernel(*refs):
    parts, (q, out, buf, sem) = refs[:-4], refs[-4:]
    e = parts[0][...]
    for p in parts[1:]:
        e = e + p[...].astype(F32)
    gain = 2.0 * math.sqrt(YF / M)
    e = e.astype(BF)
    turned = jnp.concatenate([e[:, M:], -e[:, :M]], 1)
    width = 512
    copies = []
    for i in range(YF // width):
        cols = slice(i * width, (i + 1) * width)
        buf[0, :, cols] = (dot(e, q[:, cols]) * gain).astype(BF)
        buf[1, :, cols] = (dot(turned, q[:, cols]) * gain).astype(BF)
        copies.append(pltpu.make_async_copy(buf.at[:, :, cols], out.at[0, :, :, cols], sem.at[i]))
        copies[-1].start()
    for c in copies:
        c.wait()


def bind(kernel, *args):
    def body(*refs):
        kernel(*args, *refs)

    return body


def exchange(blocks, nf):
    if len(blocks) == 1:
        return [lax.all_to_all(blocks[0], "facet", split_axis=0, concat_axis=0, tiled=True)]
    got = [lax.ppermute(blocks[i], "facet", [(z, z ^ i) for z in range(nf)]) for i in range(nf - 1, 0, -1)]
    return [blocks[0], *got[::-1]]


def gather(value):
    got = [send(value, dh, 0, ds) for dh, ds in steps()[:0:-1]]
    return [value] + got[::-1]


def shards(facets, weights, facet_offsets, subgrid_offsets, column):
    planes = facets[0]
    rows_here = planes.shape[1]
    block_rows, sub_here, _ = weights.shape
    nf = facet_offsets.shape[0]
    high, low, sub = team_layout()
    group = high * sub
    offs = jnp.transpose(facet_offsets)
    limit = 20 << 20 if nf <= 4 else 56 << 20
    side = sub_here * M
    wide = (rows_here, 2 * M)
    hold = [pltpu.VMEM(planes.shape, BF), pltpu.SemaphoreType.DMA((YF // 512,))]

    q, a = call(
        a_kernel,
        "facet_columns",
        (column, planes),
        [((2 * M, YF), BF), (wide, BF)],
        [smem(), hbm()],
        hold,
        flops=8 * rows_here * YF * M,
        limit=limit,
    )
    blocks = gather(a)
    shape = (low * side, group * rows_here)
    p_re, p_im = call(
        bind(p_kernel, sub_here, rows_here),
        "p_table",
        (subgrid_offsets,),
        [(shape, BF), (shape, BF)],
        [smem()],
        flops=1 << 29,
        limit=limit,
    )
    r, w = call(
        bind(row_kernel, block_rows),
        "row_table",
        (offs,),
        [((2, XM, 2 * M), BF), ((2 * M, XM), BF)],
        [smem()],
        flops=1 << 28,
        limit=limit,
    )
    (col,) = call(
        col_kernel,
        "col_table",
        (offs,),
        [((nf * 2 * M, 2 * XM), BF)],
        [smem()],
        flops=1 << 29,
        limit=limit,
    )
    shape = (low * rows_here, group * side)
    pt_re, pt_im = call(
        bind(pt_kernel, sub_here, rows_here),
        "pt_table",
        (subgrid_offsets,),
        [(shape, BF), (shape, BF)],
        [smem()],
        [pltpu.VMEM((rows_here, M), F32)],
        flops=1 << 29,
        limit=limit,
    )
    parts = []
    for p in [*range(1, low), 0]:
        (c,) = call(
            bind(c_kernel, sub_here, p),
            f"contrib_{p}",
            (*blocks, p_re, p_im),
            [((2 * M, side), BF if p else F32)],
            [vmem()] * (group + 2),
            flops=8 * side * group * rows_here * M,
            limit=limit,
        )
        parts.append(send(c, 0, (low - p) % low, 0) if p else c)
    parts = parts[-1:] + parts[:-1]
    pieces = [((block_rows, 2 * M), BF)] * nf if by_permutes(nf) else [((nf, block_rows, 2 * M), BF)]
    count = len(pieces)
    groups = XM // 128
    weights = weights.reshape(block_rows, sub_here, groups, 128).transpose(0, 2, 1, 3).reshape(-1, 128)
    spectra, ds = [], []
    ks = []
    for s in range(sub_here):
        k = call(
            bind(k_kernel, low, s),
            f"row_spectra_{s}",
            (*parts, r),
            pieces,
            [vmem()] * (low + 1),
            flops=8 * XM * M * M,
            limit=limit,
        )
        ks.append(exchange(k, nf))
    ys = []
    for s in range(sub_here):
        spectrum, *y = call(
            bind(spectrum_kernel, count, s, sub_here),
            f"spectrum_{s}",
            (*ks[s], weights, col),
            [((2, block_rows, XM), F32), *pieces],
            [vmem()] * (count + 2),
            flops=16 * block_rows * nf * M * XM,
            limit=limit,
        )
        spectra.append(spectrum)
        ys.append(exchange(y, nf))
    for s in range(sub_here):
        (d,) = call(
            d_kernel,
            f"windows_{s}",
            (*ys[s], w),
            [((M, 2 * M), BF)],
            [vmem()] * (count + 1),
            flops=8 * XM * M * M,
            limit=limit,
        )
        ds.append(gather(d))
    blocks = [ds[s][i] for i in range(group) for s in range(sub_here)]
    shape = (block_rows * sub_here * groups * 2, 128)
    (spectra,) = call(
        spread_kernel,
        "spread",
        spectra,
        [(shape, F32)],
        [vmem()] * sub_here,
        [pltpu.VMEM(shape, F32), pltpu.SemaphoreType.DMA(())],
        flops=1 << 29,
        limit=limit,
        out_spec=hbm,
    )
    spectra = spectra.reshape(block_rows, sub_here, groups, 2, 128).transpose(0, 1, 3, 2, 4)
    parts = []
    for p in [*range(1, low), 0]:
        (e,) = call(
            bind(e_kernel, p, sub_here),
            f"rows_{p}",
            (*blocks, pt_re, pt_im),
            [(wide, BF if p else F32)],
            [vmem()] * (len(blocks) + 2),
            flops=8 * rows_here * group * side * M,
            limit=limit,
        )
        parts.append(send(e, 0, (low - p) % low, 0) if p else e)
    parts = parts[-1:] + parts[:-1]
    (update,) = call(
        update_kernel,
        "facet_update",
        (*parts, q),
        [((1, 2, rows_here, YF), BF)],
        [vmem()] * (low + 1),
        hold,
        flops=8 * rows_here * YF * M,
        limit=limit,
        out_spec=hbm,
    )
    return (update, spectra.reshape(block_rows, sub_here, 2, XM))


def solution(mesh):
    return jax.shard_map(
        shards,
        mesh=mesh,
        in_specs=(
            P("facet", None, ("half", "sub"), None),
            P("facet", ("half", "sub"), None),
            P(),
            P(),
            P(),
        ),
        out_specs=(
            P("facet", None, ("half", "sub"), None),
            P("facet", ("half", "sub"), None, None),
        ),
        check_vma=False,
    )
```
